32 devices in a mesh: fx: 4 (over z), fy: 4 (over x, core), fz: 2 (over y).
Axes of the slice: x: 2, y: 2, z: 4, core: 2. Of those that a mesh axis runs over, the one named last changes fastest.
Arguments:
- pressure: float32 [128, 512, 256], P('fx', 'fy', 'fz'), may hold values from -6 to 6
- source: float32 [128, 512, 256], P('fx', 'fy', 'fz'), may hold values from -6 to 6
- diag_shift: float32 [128, 512, 256], P('fx', 'fy', 'fz'), may hold values from 0.1 to 2
- iface_cells: int32 [262144], P(('fx', 'fy', 'fz')), may hold values from 0 to 524287
- iface_coef: float32 [262144], P(('fx', 'fy', 'fz')), may hold values from -6 to 6
- iface_xyz: float32 [3, 262144], P(None, ('fx', 'fy', 'fz')), may hold values from -6 to 6
- node_xyz: float32 [3, 65536], P(None, ('fx', 'fy', 'fz')), may hold values from -6 to 6
- owners: int32 [2048], P(('fx', 'fy', 'fz')), may hold values from 0 to 31, as said below
- node_lists: int32 [65536, 8], P(('fx', 'fy', 'fz')), may hold values from 0 to 1048575
Outputs:
- new_pressure: float32 [128, 512, 256], P('fx', 'fy', 'fz')
- node_loads: float32 [65536], P(('fx', 'fy', 'fz'))
The draws below stay inside these ranges and needn't reach their ends.
Inputs may be any that keep to these rules, and one draw needn't show every extreme that they name: `owners`: among the 64 tiles of one device, at most 4 have the same owner; one device owns exactly 4 tiles of every device's block; every device owns at least one tile.
All inputs are finite; a program needn't handle non-finite values.
Results may differ from the reference program's by a relative error of at most 0.0003.
Values sent between devices are 32-bit elements; how exact they have to be, the bound alone decides.
No kernel may reach another device: no remote copies, remote signals or barrier semaphores. Data moves between devices by JAX's collectives and lax.ppermute only.
A program may use at most 192 MiB of HBM per device.

```python
import math
import jax
import jax.numpy as jnp
from jax import lax

CX = 32
CY = 128
CZ = 128
ITERS = 4
TILE = 128
CAP = 4
NODE_DEV = 2048
NEIGH = 8
OWNERS = 32
TILES_DEV = 64
NX = 128
NY = 512
NZ = 256
NTILES = 2048
NPTS = 262144
NODES = 65536
N_FY = 4
N_FZ = 2


def draw_owners(key, part):
    key_heavy, key_jitter, key_order = jax.random.split(jax.random.fold_in(key, 7031), 3)
    heavy = jax.random.randint(key_heavy, (), 0, OWNERS)
    jitter = jax.random.randint(key_jitter, (OWNERS,), 0, CAP)
    cycle_len = (OWNERS - 1) * CAP
    window = TILES_DEV - CAP
    senders = jnp.arange(OWNERS, dtype=jnp.int32)
    starts = senders * window + jitter
    spots = (starts[:, None] + jnp.arange(window, dtype=jnp.int32)[None, :]) % cycle_len
    others = (heavy + 1 + spots // CAP) % OWNERS
    heavy_part = jnp.zeros((OWNERS, CAP), jnp.int32) + heavy
    table = jnp.concatenate([heavy_part, others.astype(jnp.int32)], axis=1)
    scores = jax.random.randint(key_order, (OWNERS, TILES_DEV), 0, 1048576) * TILES_DEV
    scores = scores + jnp.arange(TILES_DEV, dtype=jnp.int32)[None, :]
    shuffle = jnp.argsort(scores, axis=1, stable=True)
    table = jnp.take_along_axis(table, shuffle, axis=1)
    return table.reshape(-1).astype(jnp.int32)


def set_ends(drawn, own_key, smallest, high):
    longest = drawn.shape.index(max(drawn.shape))
    spots = []
    for shift in (0, 1):
        where = [jax.random.randint(jax.random.fold_in(own_key, axis), (), 0, length) for axis, length in enumerate(drawn.shape)]
        where[longest] = (where[longest] + shift) % drawn.shape[longest]
        spots.append(tuple(where))
    return drawn.at[spots[0]].set(smallest).at[spots[1]].set(high)


def block_levels(own_key, dims, cuts, least, largest):
    level, own = 1.0, jax.random.fold_in(own_key, 6)
    for axis_at, shards_of in cuts:
        heights = jnp.exp(jax.random.uniform(jax.random.fold_in(own, axis_at), (shards_of,), jnp.float32, least / len(cuts), largest / len(cuts)))
        level = level * jnp.repeat(heights, dims[axis_at] // shards_of).reshape([-1 if axis == axis_at else 1 for axis in range(len(dims))])
    return level


def noise(rng, dims, spread, most, cuts=(), kind=jnp.bfloat16):
    array = jax.random.normal(rng, dims, jnp.float32) * spread
    if len(cuts) > 0:
        array = block_levels(rng, dims, cuts, -0.22, 0.18) * array
    return jnp.clip(array, min=-most, max=most).astype(kind)


def setup_inputs(seed: int = 0) -> dict:
    key_of = jax.random.split(jax.random.key(seed), 10)
    pressure = noise(key_of[0], (NX, NY, NZ), 1.0, 6.0, ((0, 4), (1, 4), (2, 2)), jnp.float32)
    source = noise(key_of[1], (NX, NY, NZ), 1.0, 6.0, ((0, 4), (1, 4), (2, 2)), jnp.float32)
    diag_shift = jnp.clip(jnp.exp(math.log(2.0) - 2.9957323 * jax.random.uniform(key_of[2], (NX, NY, NZ), jnp.float32) ** block_levels(key_of[2], (NX, NY, NZ), ((0, 4), (1, 4), (2, 2)), -0.2, 0.2)), 0.1, 2.0)
    iface_cells = set_ends(jax.random.randint(key_of[3], (NPTS,), 0, CX * CY * CZ), jax.random.fold_in(key_of[3], 1), 0, (CX * CY * CZ) - 1).astype(jnp.int32)
    iface_coef = noise(key_of[4], (NPTS,), 1.0, 6.0, ((0, 32),), jnp.float32)
    iface_xyz = noise(key_of[5], (3, NPTS), 1.0, 6.0, ((1, 32),), jnp.float32)
    node_xyz = noise(key_of[6], (3, NODES), 1.0, 6.0, ((1, 32),), jnp.float32)
    owners = draw_owners(jax.random.fold_in(key_of[9], 71), 0)
    node_lists = set_ends(jax.random.randint(key_of[8], (NODES, NEIGH), 0, 1048576), jax.random.fold_in(key_of[8], 1), 0, 1048575).astype(jnp.int32)
    return dict(pressure=pressure, source=source, diag_shift=diag_shift, iface_cells=iface_cells, iface_coef=iface_coef, iface_xyz=iface_xyz, node_xyz=node_xyz, owners=owners, node_lists=node_lists)


GAUSS_RATE = 0.5


def jacobi_step(pressure_now, source, diag_shift):
    neighbours = jnp.roll(pressure_now, 1, 0) + jnp.roll(pressure_now, -1, 0)
    neighbours = neighbours + jnp.roll(pressure_now, 1, 1) + jnp.roll(pressure_now, -1, 1)
    neighbours = neighbours + jnp.roll(pressure_now, 1, 2) + jnp.roll(pressure_now, -1, 2)
    return (neighbours + source) / (6.0 + diag_shift)


def reference(pressure, source, diag_shift, iface_cells, iface_coef, iface_xyz, node_xyz, owners, node_lists):
    points = jnp.arange(NPTS, dtype=jnp.int32)
    holder = points // (TILES_DEV * TILE)
    block_x = holder // (N_FY * N_FZ)
    block_y = (holder // N_FZ) % N_FY
    block_z = holder % N_FZ
    cell_x = block_x * CX + iface_cells // (CY * CZ)
    cell_y = block_y * CY + (iface_cells // CZ) % CY
    cell_z = block_z * CZ + iface_cells % CZ
    values = iface_coef * pressure[cell_x, cell_y, cell_z]
    pressure_now = pressure
    for sweep_index in range(ITERS):
        pressure_now = jacobi_step(pressure_now, source, diag_shift)
    counts = jnp.bincount(owners, length=OWNERS).astype(jnp.int32)
    grouped = jnp.argsort(owners, stable=True).astype(jnp.int32)
    offsets = (jnp.cumsum(counts) - counts).astype(jnp.int32)
    tile_values = values.reshape(NTILES, TILE)
    tile_xyz = iface_xyz.reshape(3, NTILES, TILE)

    def one_owner(inputs):
        owner_id, coords, entries = inputs
        chosen = grouped[offsets[owner_id] + entries % counts[owner_id]]
        distance = jnp.zeros((NODE_DEV, NEIGH, TILE), jnp.float32)
        for component in range(3):
            gap_axis = coords[component][:, None, None] - tile_xyz[component][chosen]
            distance = distance + gap_axis * gap_axis
        return jnp.sum(jnp.exp(-GAUSS_RATE * distance) * tile_values[chosen], axis=(1, 2))

    owner_ids = jnp.arange(OWNERS, dtype=jnp.int32)
    node_coords = node_xyz.reshape(3, OWNERS, NODE_DEV).transpose(1, 0, 2)
    node_entries = node_lists.reshape(OWNERS, NODE_DEV, NEIGH)
    node_loads = lax.map(one_owner, (owner_ids, node_coords, node_entries))
    return pressure_now, node_loads.reshape(NODES)
```

```python
import functools

import jax
import jax.numpy as jnp
from jax import lax
from jax.experimental import pallas as pl
from jax.experimental.pallas import tpu as pltpu
from jax.sharding import PartitionSpec as P

ITERS = 4
CAP = 4
LANES = 128
SUBLANES = 8
GAUSS_RATE = 0.5
AXES = ("fx", "fy", "fz")
F32 = jnp.float32


def vmem():
    return pl.BlockSpec(memory_space=pltpu.VMEM)


def smem():
    return pl.BlockSpec(memory_space=pltpu.SMEM)


def params(mib):
    return pltpu.CompilerParams(vmem_limit_bytes=mib * 1024 * 1024)


def shape_of(*dims):
    return jax.ShapeDtypeStruct(dims, F32)


def z_pack_dims(cx, cy):
    per = cy // SUBLANES
    planes = LANES // per
    return per, planes, cx // planes


def pack_z(plane, x, zf_ref, per, planes):
    cy = plane.shape[0]
    lane = lax.broadcasted_iota(jnp.int32, (cy, LANES), 1)
    row = lax.broadcasted_iota(jnp.int32, (cy, LANES), 0)
    mine = lane == row // SUBLANES
    shift = (x % planes) * per
    for side, col in ((0, 0), (1, LANES - 1)):
        spread = jnp.broadcast_to(plane[:, col : col + 1], (cy, LANES))
        kept = jnp.where(mine, spread, 0.0).reshape(per, SUBLANES, LANES)
        moved = pltpu.roll(jnp.sum(kept, axis=0), shift, 1)
        zf_ref[side, x // planes] = zf_ref[side, x // planes] + moved


def unpack_z(packed, x, per, planes):
    back = (LANES - (x % planes) * per) % LANES
    rolled = pltpu.roll(packed, back, 1)
    parts = [jnp.broadcast_to(rolled[:, j : j + 1], (SUBLANES, LANES)) for j in range(per)]
    return jnp.concatenate(parts, axis=0)


def emit_y(plane, x, ylo_ref, yhi_ref):
    ylo_ref[pl.ds(x, 1), :] = plane[0:1]
    yhi_ref[pl.ds(x, 1), :] = plane[plane.shape[0] - 1 :]


def faces_kernel(p_ref, ylo_ref, yhi_ref, zf_ref):
    cx, cy, _ = p_ref.shape
    per, planes, _ = z_pack_dims(cx, cy)
    zf_ref[...] = jnp.zeros(zf_ref.shape, F32)

    def step(x, carry):
        plane = p_ref[x]
        emit_y(plane, x, ylo_ref, yhi_ref)
        pack_z(plane, x, zf_ref, per, planes)
        return carry

    lax.fori_loop(0, cx, step, 0)


def sweep_kernel(first, last, swap, *refs):
    p_ref, src_ref, inv_in_ref, xlo_ref, xhi_ref, ylo_ref, yhi_ref, zr_ref = refs[:8]
    outs = refs[8:]
    out_ref = outs[0]
    outs = outs[1:]
    if first:
        inv_out_ref = outs[0]
        outs = outs[1:]
    cx, cy, cz = p_ref.shape
    per, planes, _ = z_pack_dims(cx, cy)
    zlo_at, zhi_at = (1, 0) if swap else (0, 1)
    if not last:
        xlo_out, xhi_out, ylo_out, yhi_out, zf_ref = outs
        zf_ref[...] = jnp.zeros(zf_ref.shape, F32)
    lane = lax.broadcasted_iota(jnp.int32, (cy, cz), 1)

    def one(x, below, above):
        here = p_ref[x]
        total = below + above
        total = total + jnp.concatenate([ylo_ref[pl.ds(x, 1), :], here[: cy - 1]], axis=0)
        total = total + jnp.concatenate([here[1:], yhi_ref[pl.ds(x, 1), :]], axis=0)
        zlo = unpack_z(zr_ref[zlo_at, x // planes], x, per, planes)
        zhi = unpack_z(zr_ref[zhi_at, x // planes], x, per, planes)
        total = total + jnp.where(lane == 0, zlo, pltpu.roll(here, 1, 1))
        total = total + jnp.where(lane == cz - 1, zhi, pltpu.roll(here, cz - 1, 1))
        if first:
            inv = 1.0 / (6.0 + inv_in_ref[x])
            inv_out_ref[x] = inv
        else:
            inv = inv_in_ref[x]
        result = (total + src_ref[x]) * inv
        out_ref[x] = result
        if not last:
            emit_y(result, x, ylo_out, yhi_out)
            pack_z(result, x, zf_ref, per, planes)
        return result

    result = one(0, xlo_ref[0], p_ref[1])
    if not last:
        xlo_out[0] = result

    def step(x, carry):
        one(x, p_ref[x - 1], p_ref[x + 1])
        return carry

    lax.fori_loop(1, cx - 1, step, 0)
    result = one(cx - 1, p_ref[cx - 2], xhi_ref[0])
    if not last:
        xhi_out[0] = result


def gather_kernel(row_ref, target_ref, p_ref, lane_ref, coef_ref, xyz_ref, out_ref):
    tiles, width = coef_ref.shape
    out_ref[...] = jnp.zeros(out_ref.shape, F32)
    sub = lax.broadcasted_iota(jnp.int32, (SUBLANES, LANES), 0)
    lane = lax.broadcasted_iota(jnp.int32, (SUBLANES, LANES), 1)

    def tile_step(t, carry):
        pick = jnp.broadcast_to(lane_ref[pl.ds(t, 1), :], (SUBLANES, LANES))
        total = jnp.zeros((SUBLANES, LANES), F32)
        for group in range(width // SUBLANES):
            rows = None
            for s in range(SUBLANES):
                at = row_ref[t * width + group * SUBLANES + s]
                row = jnp.broadcast_to(p_ref[pl.ds(at, 1), :], (SUBLANES, LANES))
                rows = row if rows is None else jnp.where(sub == s, row, rows)
            picked = jnp.take_along_axis(rows, pick, axis=1, mode="promise_in_bounds")
            total = jnp.where(lane == sub + group * SUBLANES, picked, total)
        values = jnp.sum(total, axis=0, keepdims=True) * coef_ref[pl.ds(t, 1), :]
        slot = target_ref[t]
        out_ref[slot, 0:1, :] = values
        for c in range(3):
            out_ref[slot, c + 1 : c + 2, :] = xyz_ref[c, pl.ds(t, 1), :]
        return carry

    lax.fori_loop(0, tiles, tile_step, 0)


def lane_gather(row, chunks, low, high):
    got = None
    for at in range(chunks):
        part = jnp.broadcast_to(row[:, at * LANES : (at + 1) * LANES], (SUBLANES, LANES))
        part = jnp.take_along_axis(part, low, axis=1, mode="promise_in_bounds")
        got = part if got is None else jnp.where(high == at, part, got)
    return got


def node_kernel(inc_ref, wanted_ref, slot_ref, node_ref, out_ref, table_ref):
    slots = inc_ref.shape[0]
    width = inc_ref.shape[2]
    neigh, rows, _ = wanted_ref.shape
    chunks = slots // LANES
    scale = GAUSS_RATE ** 0.5
    for c in range(4):
        part = inc_ref[:, c, :]
        if c > 0:
            part = part * scale
        table_ref[c] = part.T
    slot_row = slot_ref[...]

    def pair(step, carry):
        k = step % neigh
        block = step // neigh
        at = pl.ds(pl.multiple_of(block * SUBLANES, SUBLANES), SUBLANES)
        wanted = wanted_ref[k, at, :]
        chosen = lane_gather(slot_row, chunks, wanted % LANES, wanted // LANES)
        low = chosen % LANES
        high = chosen // LANES
        coords = [node_ref[c, at, :] * scale for c in range(3)]
        before = jnp.where(k == 0, 0.0, out_ref[at, :])

        def points(base, total):
            for u in range(16):
                p = base * 16 + u
                got = [
                    lane_gather(table_ref[c, pl.ds(p, 1), :], chunks, low, high) for c in range(4)
                ]
                gaps = [coords[c] - got[c + 1] for c in range(3)]
                dist = gaps[0] * gaps[0] + gaps[1] * gaps[1] + gaps[2] * gaps[2]
                total = total + jnp.exp(-dist) * got[0]
            return total

        out_ref[at, :] = lax.fori_loop(0, width // 16, points, before)
        return carry

    lax.fori_loop(0, neigh * (rows // SUBLANES), pair, 0)


def ring(axis, up):
    count = lax.axis_size(axis)
    if up:
        return [(i, (i + 1) % count) for i in range(count)]
    return [((i + 1) % count, i) for i in range(count)]


def exchange(xlo, xhi, ylo, yhi, zf):
    from_x_lo = lax.ppermute(xhi, "fx", ring("fx", True))
    from_x_hi = lax.ppermute(xlo, "fx", ring("fx", False))
    from_y_lo = lax.ppermute(yhi, "fy", ring("fy", True))
    from_y_hi = lax.ppermute(ylo, "fy", ring("fy", False))
    if lax.axis_size("fz") == 2:
        z = lax.ppermute(zf, "fz", ring("fz", True))
    else:
        z = jnp.stack(
            [
                lax.ppermute(zf[1], "fz", ring("fz", True)),
                lax.ppermute(zf[0], "fz", ring("fz", False)),
            ]
        )
    return from_x_lo, from_x_hi, from_y_lo, from_y_hi, z


def on_device(
    pressure, source, diag_shift, iface_cells, iface_coef, iface_xyz, node_xyz, owners, node_lists
):
    devices = lax.axis_size(AXES)
    cx, cy, cz = pressure.shape
    tiles_dev = owners.shape[0]
    width = iface_coef.shape[0] // tiles_dev
    node_count, neigh = node_lists.shape
    slots = devices * CAP
    per, planes, packs = z_pack_dims(cx, cy)
    y_shape = shape_of(cx, cz)
    z_shape = shape_of(2, packs, SUBLANES, LANES)
    x_shape = shape_of(1, cy, cz)
    block = shape_of(cx, cy, cz)

    owned_by = (owners[:, None] == jnp.arange(devices, dtype=jnp.int32)[None, :]).astype(jnp.int32)
    order = lax.broadcasted_iota(jnp.int32, (tiles_dev, tiles_dev), 0)
    other = lax.broadcasted_iota(jnp.int32, (tiles_dev, tiles_dev), 1)
    same = (owners[:, None] == owners[None, :]) & (other < order)
    target = owners * CAP + jnp.sum(same.astype(jnp.int32), axis=1)
    counts = jnp.sum(owned_by, axis=0)
    filled = (jnp.arange(CAP, dtype=jnp.int32)[None, :] < counts[:, None]).astype(F32)
    arrived = lax.all_to_all(filled, AXES, split_axis=0, concat_axis=0, tiled=True)
    arrived = arrived.reshape(slots).astype(jnp.int32)
    lower = lax.broadcasted_iota(jnp.int32, (slots, slots), 1) <= lax.broadcasted_iota(
        jnp.int32, (slots, slots), 0
    )
    prefix = jnp.sum(jnp.where(lower, arrived[None, :], 0), axis=1)
    owned_count = jnp.sum(arrived)
    entry = jnp.arange(slots, dtype=jnp.int32)
    hit = (prefix[None, :] == entry[:, None] + 1) & (arrived[None, :] > 0)
    slot_of = jnp.sum(jnp.where(hit, entry[None, :], 0), axis=1).reshape(1, slots)
    wanted = (node_lists.T % owned_count).reshape(neigh, node_count // LANES, LANES)

    ylo, yhi, zf = pl.pallas_call(
        faces_kernel,
        out_shape=(y_shape, y_shape, z_shape),
        in_specs=[vmem()],
        out_specs=(vmem(),) * 3,
        compiler_params=params(8),
        name="faces",
    )(pressure)
    halos = exchange(pressure[:1], pressure[cx - 1 :], ylo, yhi, zf)

    outgoing = pl.pallas_call(
        gather_kernel,
        out_shape=shape_of(slots, 4, width),
        in_specs=[smem(), smem(), vmem(), vmem(), vmem(), vmem()],
        out_specs=vmem(),
        compiler_params=params(12),
        name="cells",
    )(
        iface_cells // cz,
        target,
        pressure.reshape(cx * cy, cz),
        (iface_cells % cz).reshape(tiles_dev, width),
        iface_coef.reshape(tiles_dev, width),
        iface_xyz.reshape(3, tiles_dev, width),
    )
    incoming = lax.all_to_all(outgoing, AXES, split_axis=0, concat_axis=0, tiled=True)

    swap = lax.axis_size("fz") == 2
    current, inverse = pressure, diag_shift
    for index in range(ITERS):
        first, last = index == 0, index == ITERS - 1
        shapes = [block]
        if first:
            shapes.append(block)
        if not last:
            shapes += [x_shape, x_shape, y_shape, y_shape, z_shape]
        results = pl.pallas_call(
            functools.partial(sweep_kernel, first, last, swap),
            out_shape=tuple(shapes),
            in_specs=[vmem()] * 8,
            out_specs=tuple(vmem() for _ in shapes),
            compiler_params=params(16),
            name="sweep",
        )(current, source, inverse, *halos)
        current = results[0]
        if first:
            inverse = results[1]
        if not last:
            halos = exchange(*results[-5:])

    loads = pl.pallas_call(
        node_kernel,
        out_shape=shape_of(node_count // LANES, LANES),
        in_specs=[vmem()] * 4,
        out_specs=vmem(),
        scratch_shapes=[pltpu.VMEM((4, width, slots), F32)],
        compiler_params=params(12),
        name="nodes",
    )(incoming, wanted, slot_of, node_xyz.reshape(3, node_count // LANES, LANES))
    return current, loads.reshape(node_count)


def solution(mesh):
    placed = (
        P("fx", "fy", "fz"),
        P("fx", "fy", "fz"),
        P("fx", "fy", "fz"),
        P(AXES),
        P(AXES),
        P(None, AXES),
        P(None, AXES),
        P(AXES),
        P(AXES, None),
    )
    return jax.shard_map(
        on_device,
        mesh=mesh,
        in_specs=placed,
        out_specs=(P("fx", "fy", "fz"), P(AXES)),
        check_vma=False,
    )
```

```python
import functools

import jax
import jax.numpy as jnp
from jax import lax
from jax.experimental import pallas as pl
from jax.experimental.pallas import tpu as pltpu
from jax.sharding import PartitionSpec as P

ITERS = 4
CAP = 4
LANES = 128
SUBLANES = 8
GAUSS_RATE = 0.5
AXES = ("fx", "fy", "fz")
F32 = jnp.float32


def vmem():
    return pl.BlockSpec(memory_space=pltpu.VMEM)


def hbm():
    return pl.BlockSpec(memory_space=pltpu.HBM)


def smem():
    return pl.BlockSpec(memory_space=pltpu.SMEM)


def params(mib):
    return pltpu.CompilerParams(vmem_limit_bytes=mib * 1024 * 1024)


def shape_of(*dims):
    return jax.ShapeDtypeStruct(dims, F32)


def z_pack_dims(cx, cy):
    per = cy // SUBLANES
    planes = LANES // per
    return per, planes, cx // planes


def edge_z(side, plane, offset, packed, lane):
    col = 0 if side == 0 else LANES - 1
    for j in range(plane.shape[0] // SUBLANES):
        part = plane[j * SUBLANES : (j + 1) * SUBLANES, col : col + 1]
        spread = jnp.broadcast_to(part, (SUBLANES, LANES))
        packed = spread if packed is None else jnp.where(lane == offset + j, spread, packed)
    return packed


def column_z(packed, offset, per):
    parts = [
        jnp.broadcast_to(packed[:, offset + j : offset + j + 1], (SUBLANES, LANES))
        for j in range(per)
    ]
    return jnp.concatenate(parts, axis=0)


def emit_y(plane, x, ylo_ref, yhi_ref):
    ylo_ref[pl.ds(x, 1), :] = plane[0:1]
    yhi_ref[pl.ds(x, 1), :] = plane[plane.shape[0] - 1 :]


def faces_kernel(p_ref, copy_ref, xlo_ref, xhi_ref, ylo_ref, yhi_ref, zf_ref):
    cx, cy, _ = p_ref.shape
    per, planes, packs = z_pack_dims(cx, cy)
    lane = lax.broadcasted_iota(jnp.int32, (SUBLANES, LANES), 1)
    xlo_ref[0] = p_ref[0]
    xhi_ref[0] = p_ref[cx - 1]

    def step(block, carry):
        packed = [None, None]
        for u in range(planes):
            x = block * planes + u
            plane = p_ref[x]
            copy_ref[x] = plane
            emit_y(plane, x, ylo_ref, yhi_ref)
            for side in range(2):
                packed[side] = edge_z(side, plane, u * per, packed[side], lane)
        zf_ref[0, block] = packed[0]
        zf_ref[1, block] = packed[1]
        return carry

    lax.fori_loop(0, packs, step, 0)


def sweep_kernel(first, last, swap, *refs):
    p_ref, src_ref, inv_in_ref, xlo_ref, xhi_ref, ylo_ref, yhi_ref, zr_ref = refs[:8]
    outs = refs[8:]
    out_ref = outs[0]
    outs = outs[1:]
    if first:
        inv_out_ref = outs[0]
        outs = outs[1:]
    cx, cy, cz = p_ref.shape
    per, planes, packs = z_pack_dims(cx, cy)
    zlo_at, zhi_at = (1, 0) if swap else (0, 1)
    if not last:
        xlo_out, xhi_out, ylo_out, yhi_out, zf_ref = outs
    lane = lax.broadcasted_iota(jnp.int32, (cy, cz), 1)
    small_lane = lax.broadcasted_iota(jnp.int32, (SUBLANES, LANES), 1)

    def step(block, carry):
        packed = [None, None]
        zlo_pack = zr_ref[zlo_at, block]
        zhi_pack = zr_ref[zhi_at, block]
        for u in range(planes):
            x = block * planes + u
            if u == 0:
                below = jnp.where(block == 0, xlo_ref[0], p_ref[jnp.maximum(x - 1, 0)])
            else:
                below = p_ref[x - 1]
            if u == planes - 1:
                above = jnp.where(block == packs - 1, xhi_ref[0], p_ref[jnp.minimum(x + 1, cx - 1)])
            else:
                above = p_ref[x + 1]
            here = p_ref[x]
            total = below + above
            total = total + jnp.concatenate([ylo_ref[pl.ds(x, 1), :], here[: cy - 1]], axis=0)
            total = total + jnp.concatenate([here[1:], yhi_ref[pl.ds(x, 1), :]], axis=0)
            zlo = column_z(zlo_pack, u * per, per)
            zhi = column_z(zhi_pack, u * per, per)
            total = total + jnp.where(lane == 0, zlo, pltpu.roll(here, 1, 1))
            total = total + jnp.where(lane == cz - 1, zhi, pltpu.roll(here, cz - 1, 1))
            if first:
                inv = 1.0 / (6.0 + inv_in_ref[x])
                inv_out_ref[x] = inv
            else:
                inv = inv_in_ref[x]
            result = (total + src_ref[x]) * inv
            out_ref[x] = result
            if not last:
                emit_y(result, x, ylo_out, yhi_out)
                for side in range(2):
                    packed[side] = edge_z(side, result, u * per, packed[side], small_lane)
        if not last:
            zf_ref[0, block] = packed[0]
            zf_ref[1, block] = packed[1]
        return carry

    lax.fori_loop(0, packs, step, 0)
    if not last:
        xlo_out[0] = out_ref[0]
        xhi_out[0] = out_ref[cx - 1]


FAR = 100.0


def gather_kernel(
    row_ref, target_ref, p_ref, lane_ref, coef_ref, xyz_ref, src_ref, diag_ref,
    out_ref, src_out, diag_out, sems,
):
    copies = [
        pltpu.make_async_copy(src_ref, src_out, sems.at[0]),
        pltpu.make_async_copy(diag_ref, diag_out, sems.at[1]),
    ]
    for copy in copies:
        copy.start()
    tiles, width = coef_ref.shape
    out_ref[...] = jnp.full(out_ref.shape, FAR, F32)
    sub = lax.broadcasted_iota(jnp.int32, (SUBLANES, LANES), 0)
    lane = lax.broadcasted_iota(jnp.int32, (SUBLANES, LANES), 1)

    def one_tile(t):
        pick = jnp.broadcast_to(lane_ref[pl.ds(t, 1), :], (SUBLANES, LANES))
        total = jnp.zeros((SUBLANES, LANES), F32)
        for group in range(width // SUBLANES):
            rows = None
            for s in range(SUBLANES):
                at = row_ref[t, group * SUBLANES + s]
                row = jnp.broadcast_to(p_ref[pl.ds(at, 1), :], (SUBLANES, LANES))
                rows = row if rows is None else jnp.where(sub == s, row, rows)
            picked = jnp.take_along_axis(rows, pick, axis=1, mode="promise_in_bounds")
            total = jnp.where(lane == sub + group * SUBLANES, picked, total)
        values = jnp.sum(total, axis=0, keepdims=True) * coef_ref[pl.ds(t, 1), :]
        slot = target_ref[t]
        out_ref[slot, 0:1, :] = values
        for c in range(3):
            out_ref[slot, c + 1 : c + 2, :] = xyz_ref[c, pl.ds(t, 1), :]

    def tile_step(pair, carry):
        one_tile(pair * 2)
        one_tile(pair * 2 + 1)
        return carry

    lax.fori_loop(0, tiles // 2, tile_step, 0)
    for copy in copies:
        copy.wait()


def lane_gather(row, chunks, low, high):
    got = None
    for at in range(chunks):
        part = jnp.broadcast_to(row[:, at * LANES : (at + 1) * LANES], (SUBLANES, LANES))
        part = jnp.take_along_axis(part, low, axis=1, mode="promise_in_bounds")
        got = part if got is None else jnp.where(high == at, part, got)
    return got


def node_kernel(inc_ref, wanted_ref, node_ref, out_ref, table_ref):
    slots = inc_ref.shape[0]
    width = inc_ref.shape[2]
    neigh, rows, _ = wanted_ref.shape
    chunks = slots // LANES
    scale = GAUSS_RATE ** 0.5
    for c in range(4):
        part = inc_ref[:, c, :]
        if c > 0:
            part = part * scale
        table_ref[c] = part.T
    half = 0.5 * FAR * scale
    row_id = lax.broadcasted_iota(jnp.int32, (slots, slots), 0).astype(F32)
    col_id = lax.broadcasted_iota(jnp.int32, (slots, slots), 1).astype(F32)
    first_row = table_ref[1, 0:1, :]
    used_row = jnp.broadcast_to(jnp.where(first_row < half, 1.0, 0.0), (slots, slots))
    used_col = jnp.where(inc_ref[:, 1, :][:, 0:1] < 0.5 * FAR, 1.0, 0.0)
    prefix = jnp.sum(jnp.where(col_id <= row_id, used_row, 0.0), axis=1, keepdims=True)
    count = jnp.max(prefix, axis=0, keepdims=True)
    place = jnp.where(prefix == col_id + 1.0, row_id, 0.0) * used_col
    slot_row = jnp.sum(place, axis=0, keepdims=True).astype(jnp.int32)
    count = jnp.broadcast_to(count, (SUBLANES, LANES))
    ratio = 1.0 / count
    span = 128 // chunks

    def pair(step, carry):
        k = step % neigh
        block = step // neigh
        at = pl.ds(pl.multiple_of(block * SUBLANES, SUBLANES), SUBLANES)
        listed = wanted_ref[k, at, :].astype(F32)
        rest = listed - jnp.floor(listed * ratio) * count
        rest = jnp.where(rest < 0.0, rest + count, rest)
        rest = jnp.where(rest >= count, rest - count, rest)
        wanted = rest.astype(jnp.int32)
        chosen = lane_gather(slot_row, chunks, wanted % LANES, wanted // LANES)
        low = chosen % LANES
        high = chosen // LANES
        coords = [node_ref[c, at, :] * scale for c in range(3)]
        before = jnp.where(k == 0, 0.0, out_ref[at, :])

        def points(base, total):
            sums = [total, None, None, None]
            for u in range(span):
                p = base * span + u
                got = [
                    lane_gather(table_ref[c, pl.ds(p, 1), :], chunks, low, high) for c in range(4)
                ]
                gaps = [coords[c] - got[c + 1] for c in range(3)]
                dist = gaps[0] * gaps[0] + gaps[1] * gaps[1] + gaps[2] * gaps[2]
                term = jnp.exp(-dist) * got[0]
                sums[u % 4] = term if sums[u % 4] is None else sums[u % 4] + term
            return (sums[0] + sums[1]) + (sums[2] + sums[3])

        if width == span:
            out_ref[at, :] = points(0, before)
        else:
            out_ref[at, :] = lax.fori_loop(0, width // span, points, before)
        return carry

    lax.fori_loop(0, neigh * (rows // SUBLANES), pair, 0)


def ring(axis, up):
    count = lax.axis_size(axis)
    if up:
        return [(i, (i + 1) % count) for i in range(count)]
    return [((i + 1) % count, i) for i in range(count)]


def exchange(xlo, xhi, ylo, yhi, zf):
    from_x_lo = lax.ppermute(xhi, "fx", ring("fx", True))
    from_x_hi = lax.ppermute(xlo, "fx", ring("fx", False))
    from_y_lo = lax.ppermute(yhi, "fy", ring("fy", True))
    from_y_hi = lax.ppermute(ylo, "fy", ring("fy", False))
    if lax.axis_size("fz") == 2:
        z = lax.ppermute(zf, "fz", ring("fz", True))
    else:
        z = jnp.stack(
            [
                lax.ppermute(zf[1], "fz", ring("fz", True)),
                lax.ppermute(zf[0], "fz", ring("fz", False)),
            ]
        )
    return from_x_lo, from_x_hi, from_y_lo, from_y_hi, z


def on_device(
    pressure, source, diag_shift, iface_cells, iface_coef, iface_xyz, node_xyz, owners, node_lists
):
    devices = lax.axis_size(AXES)
    cx, cy, cz = pressure.shape
    tiles_dev = owners.shape[0]
    width = iface_coef.shape[0] // tiles_dev
    node_count, neigh = node_lists.shape
    slots = devices * CAP
    per, planes, packs = z_pack_dims(cx, cy)
    y_shape = shape_of(cx, cz)
    z_shape = shape_of(2, packs, SUBLANES, LANES)
    x_shape = shape_of(1, cy, cz)
    block = shape_of(cx, cy, cz)

    order = lax.broadcasted_iota(jnp.int32, (tiles_dev, tiles_dev), 0)
    other = lax.broadcasted_iota(jnp.int32, (tiles_dev, tiles_dev), 1)
    same = (owners[:, None] == owners[None, :]) & (other < order)
    target = owners * CAP + jnp.sum(same.astype(jnp.int32), axis=1)
    listed = node_lists.T.reshape(neigh, node_count // LANES, LANES)

    current, *faces = pl.pallas_call(
        faces_kernel,
        out_shape=(block, x_shape, x_shape, y_shape, y_shape, z_shape),
        in_specs=[vmem()],
        out_specs=(vmem(),) * 6,
        compiler_params=params(8),
        name="faces",
    )(pressure)
    halos = exchange(*faces)

    outgoing, source_near, inverse = pl.pallas_call(
        gather_kernel,
        out_shape=(shape_of(slots, 4, width), block, block),
        in_specs=[smem(), smem(), vmem(), vmem(), vmem(), vmem(), hbm(), hbm()],
        out_specs=(vmem(),) * 3,
        scratch_shapes=[pltpu.SemaphoreType.DMA((2,))],
        compiler_params=params(16),
        name="cells",
    )(
        (iface_cells // cz).reshape(tiles_dev, width),
        target,
        current.reshape(cx * cy, cz),
        (iface_cells % cz).reshape(tiles_dev, width),
        iface_coef.reshape(tiles_dev, width),
        iface_xyz.reshape(3, tiles_dev, width),
        source,
        diag_shift,
    )
    incoming = lax.all_to_all(outgoing, AXES, split_axis=0, concat_axis=0, tiled=True)

    swap = lax.axis_size("fz") == 2
    for index in range(ITERS):
        first, last = index == 0, index == ITERS - 1
        shapes = [block]
        if first:
            shapes.append(block)
        if not last:
            shapes += [x_shape, x_shape, y_shape, y_shape, z_shape]
        results = pl.pallas_call(
            functools.partial(sweep_kernel, first, last, swap),
            out_shape=tuple(shapes),
            in_specs=[vmem()] * 8,
            out_specs=tuple(vmem() for _ in shapes),
            compiler_params=params(16),
            name="sweep",
        )(current, source_near, inverse, *halos)
        current = results[0]
        if first:
            inverse = results[1]
        if not last:
            halos = exchange(*results[-5:])

    loads = pl.pallas_call(
        node_kernel,
        out_shape=shape_of(node_count // LANES, LANES),
        in_specs=[vmem()] * 3,
        out_specs=vmem(),
        scratch_shapes=[pltpu.VMEM((4, width, slots), F32)],
        compiler_params=params(12),
        name="nodes",
    )(incoming, listed, node_xyz.reshape(3, node_count // LANES, LANES))
    return current, loads.reshape(node_count)


def solution(mesh):
    placed = (
        P("fx", "fy", "fz"),
        P("fx", "fy", "fz"),
        P("fx", "fy", "fz"),
        P(AXES),
        P(AXES),
        P(None, AXES),
        P(None, AXES),
        P(AXES),
        P(AXES, None),
    )
    return jax.shard_map(
        on_device,
        mesh=mesh,
        in_specs=placed,
        out_specs=(P("fx", "fy", "fz"), P(AXES)),
        check_vma=False,
    )
```
